128 devices in a mesh: chan: 8 (over x, core), tile: 16 (over z, y).
Axes of the slice: x: 4, y: 4, z: 4, core: 2. Of those that a mesh axis runs over, the one named last changes fastest.
Arguments:
- voltages: bfloat16 [8, 2, 2048, 2048], P(None, None, 'tile', 'chan'), may hold values from -16 to 16
- rfi_flags: int32 [8], P('chan'), may hold values 0 or 1
- beam_steer_index: int32 [8, 8], P('chan'), may hold values from 0 to 2047
- start_columns: int32 [8, 32], P('chan'), may hold values from 0 to 2047, as said below
Outputs:
- covariance: float32 [8, 2, 2048, 2048], P('chan', None, 'tile')
- weights: float32 [8, 8, 2, 2048], P('chan', None, None, 'tile')
The draws below stay inside these ranges and needn't reach their ends.
Inputs may be any that keep to these rules, and one draw needn't show every extreme that they name: `start_columns`: the 32 antenna numbers of one channel are distinct.
All inputs are finite; a program needn't handle non-finite values. No bound on the sum of `rfi_flags` on one device may be relied on, other than what follows from the above.
Results may differ from the reference program's by a relative error of at most 0.0003.
Values may be sent and summed in bfloat16 or wider, within the bound.
No kernel may reach another device: no remote copies, remote signals or barrier semaphores. Data moves between devices by JAX's collectives and lax.ppermute only.
A program may use at most 128 MiB of HBM per device.

```python
import math
import jax
import jax.numpy as jnp
from jax import lax

ARRAY_ELEMENTS = 2048
SNAPSHOT_COUNT = 2048
SUBSPACE_SIZE = 32
SUB_ITERS = 4
CG_ITERS = 12
BEAM_COUNT = 8
CHANNEL_COUNT = 8


def draw_start_columns(key, part):
    channel_key_set = jax.random.split(jax.random.fold_in(key, 11), CHANNEL_COUNT)
    selected_beam = jax.vmap(lambda single_key: jax.random.permutation(single_key, ARRAY_ELEMENTS)[:SUBSPACE_SIZE])(channel_key_set)
    return selected_beam.astype(jnp.int32)


def draw_voltages(key, part):
    value_key = jax.random.fold_in(key, 23)
    jitter_key = jax.random.fold_in(key, 29)
    shape_full = (CHANNEL_COUNT, 2, SNAPSHOT_COUNT, ARRAY_ELEMENTS)
    position = jnp.arange(ARRAY_ELEMENTS, dtype=jnp.float32) / (ARRAY_ELEMENTS - 1)
    jitter = jnp.exp(jax.random.uniform(jitter_key, (ARRAY_ELEMENTS,), jnp.float32, jnp.log(0.8), jnp.log(1.25)))
    amplitude = jnp.exp(jnp.log(0.7) + (jnp.log(1.6) - jnp.log(0.7)) * position) * jitter
    values = jnp.clip(jax.random.normal(value_key, shape_full, jnp.float32), -6.0, 6.0)
    return (values * amplitude).astype(jnp.bfloat16)


def plant(drawn, own_key, smallest, largest):
    longest = drawn.shape.index(max(drawn.shape))
    spots = []
    for shift in (0, 1):
        where = [jax.random.randint(jax.random.fold_in(own_key, axis), (), 0, length) for axis, length in enumerate(drawn.shape)]
        where[longest] = (where[longest] + shift) % drawn.shape[longest]
        spots.append(tuple(where))
    return drawn.at[spots[0]].set(smallest).at[spots[1]].set(largest)


def setup_inputs(seed: int = 0) -> dict:
    arg_keys = jax.random.split(jax.random.key(seed), 5)
    return {
        "voltages": draw_voltages(jax.random.fold_in(arg_keys[4], 71), 0),
        "rfi_flags": plant((jax.random.randint(arg_keys[1], (CHANNEL_COUNT,), 0, 2) < 1).astype(jnp.int32), jax.random.fold_in(arg_keys[1], 1), 0, 1),
        "beam_steer_index": plant(jax.random.randint(arg_keys[2], (CHANNEL_COUNT, BEAM_COUNT), 0, ARRAY_ELEMENTS), jax.random.fold_in(arg_keys[2], 1), 0, ARRAY_ELEMENTS - 1).astype(jnp.int32),
        "start_columns": draw_start_columns(jax.random.fold_in(arg_keys[4], 71), 0),
    }


diagonal_loading = 0.1
highest = lax.Precision.HIGHEST

def steering_table(beam_entries):
    element_index = jnp.arange(ARRAY_ELEMENTS, dtype=jnp.int32)
    steer_phases = (beam_entries[..., None] * element_index % ARRAY_ELEMENTS).astype(jnp.float32) * (2.0 * math.pi / ARRAY_ELEMENTS)
    return jnp.stack([jnp.cos(steer_phases), jnp.sin(steer_phases)], axis=-2)

def orthonormal(vectors):
    dims_in = vectors.shape
    flattened = vectors.reshape(dims_in[:-2] + (dims_in[-2] * dims_in[-1],))
    gram_matrix = jnp.einsum('...kx,...lx->...kl', flattened, flattened, precision=highest)
    factor = jnp.linalg.cholesky(gram_matrix)
    solved = lax.linalg.triangular_solve(factor, flattened, left_side=True, lower=True)
    return solved.reshape(dims_in)

def apply_rows(covariance, vectors):
    upper_half = vectors[..., 0, :]
    lower_half = vectors[..., 1, :]
    stacked = jnp.stack([jnp.stack([upper_half, -lower_half], -2), jnp.stack([lower_half, upper_half], -2)], -3)
    return jnp.einsum('...bhpa,...pra->...bhr', stacked, covariance, precision=highest)

def project(vectors, subspace):
    coefficients = jnp.einsum('...bha,...kha->...bk', vectors, subspace, precision=highest)
    return vectors - jnp.einsum('...bk,...kha->...bha', coefficients, subspace, precision=highest)

def one_channel(arguments):
    voltage_block, flag_value, beam_entries, columns = arguments
    values = voltage_block.astype(jnp.float32)
    swapped = jnp.stack([values[1], -values[0]])
    real_part = jnp.einsum('psi,psj->ij', values, values, precision=highest)
    imag_part = jnp.einsum('psi,psj->ij', swapped, values, precision=highest)
    covariance = jnp.stack([real_part, imag_part]) * (1.0 / SNAPSHOT_COUNT)
    covariance_trace = jnp.sum(jnp.diagonal(covariance[0]))
    loading_amount = diagonal_loading * covariance_trace / ARRAY_ELEMENTS
    picked = covariance[:, :, columns]
    col_real = picked[0].T
    col_imag = picked[1].T
    first_block = jnp.concatenate([jnp.stack([col_real, col_imag], 1), jnp.stack([-col_imag, col_real], 1)], 0)
    subspace = orthonormal(first_block)
    for sweep_index in range(SUB_ITERS - 1):
        subspace = orthonormal(apply_rows(covariance, subspace))
    subspace = subspace * flag_value.astype(jnp.float32)
    steering = steering_table(beam_entries)

    def cg_sweep(counter, state_tuple):
        solved_weights, residual, direction, res_norm = state_tuple
        projected = project(direction, subspace)
        mapped = apply_rows(covariance, projected)
        combined = project(mapped, subspace) + loading_amount * direction
        curvature = jnp.sum(projected * mapped, axis=(1, 2)) + loading_amount * jnp.sum(direction * direction, axis=(1, 2))
        step_size = res_norm / curvature
        solved_weights = solved_weights + step_size[:, None, None] * direction
        residual = residual - step_size[:, None, None] * combined
        new_norm = jnp.sum(residual * residual, axis=(1, 2))
        direction = residual + (new_norm / res_norm)[:, None, None] * direction
        return (solved_weights, residual, direction, new_norm)
    start_state = (jnp.zeros_like(steering), steering, steering, jnp.sum(steering * steering, axis=(1, 2)))
    solved_weights = lax.fori_loop(0, CG_ITERS, cg_sweep, start_state)[0]
    array_response = jnp.sum(steering * solved_weights, axis=(1, 2))
    weights = ARRAY_ELEMENTS * solved_weights / array_response[:, None, None]
    return (covariance, weights)

def reference(voltages, rfi_flags, beam_steer_index, start_columns):
    covariance, weights = lax.map(one_channel, (voltages, rfi_flags, beam_steer_index, start_columns))
    return (covariance, weights)
```

```python
import functools
import math

import jax
import jax.numpy as jnp
from jax import lax
from jax.experimental import pallas as pl
from jax.experimental.pallas import tpu as pltpu
from jax.sharding import Mesh
from jax.sharding import PartitionSpec as P

ARRAY_ELEMENTS = 2048
SNAPSHOT_COUNT = 2048
SUBSPACE_SIZE = 32
BEAM_COUNT = 8
SUB_ITERS = 4
CG_ITERS = 12
TILE = ("tile_0", "tile_1")
TILES = 16
ROWS = 128
WIDE = 256

diagonal_loading = 0.1
highest = lax.Precision.HIGHEST
f32 = jnp.float32
bf16 = jnp.bfloat16


def pieces(x):
    hi = x.astype(bf16)
    rest = x - hi.astype(f32)
    mid = rest.astype(bf16)
    low = (rest - mid.astype(f32)).astype(bf16)
    return jnp.concatenate([hi, mid, low], 0)


def fold(x, count):
    rows = x.shape[0] // count
    total = x[:rows]
    for n in range(1, count):
        total = total + x[n * rows : (n + 1) * rows]
    return total


def plain(a, b):
    return lax.dot_general(a, b, (((1,), (0,)), ((), ())), preferred_element_type=f32)


def turned_dot(a, b, precision=None):
    return lax.dot_general(
        a, b, (((1,), (1,)), ((), ())), preferred_element_type=f32, precision=precision
    )


def through(lhs, matrix, count, sign):
    parts = []
    for n in range(ARRAY_ELEMENTS // WIDE):
        cols = pl.ds(n * WIDE, WIDE)
        by_real = fold(plain(lhs[...], matrix[0, :, cols]), count)
        by_imag = fold(plain(lhs[...], matrix[1, :, cols]), count)
        half = by_real.shape[0] // 2
        swapped = jnp.concatenate([-by_imag[half:], by_imag[:half]], 0)
        parts.append(by_real + swapped if sign > 0 else by_real - swapped)
    return jnp.concatenate(parts, 1)


def beam_sum(x):
    folded = x[:BEAM_COUNT] + x[BEAM_COUNT:]
    return jnp.sum(folded, axis=1, keepdims=True)


def twice(x):
    return jnp.concatenate([x, x], 0)


def unit_rows(y):
    size = SUBSPACE_SIZE
    y_real, y_imag = y[:size], y[size:]
    crossed = jnp.concatenate([y_imag, -y_real], 0)
    gram = turned_dot(y, y_real, highest) + turned_dot(crossed, y_imag, highest)
    a_r, a_i = gram[:size], gram[size:]
    row = lax.broadcasted_iota(jnp.int32, (size, size), 0)
    col = lax.broadcasted_iota(jnp.int32, (size, size), 1)
    j_r = jnp.where(row == col, 1.0, 0.0).astype(f32)
    j_i = jnp.zeros((size, size), f32)
    for k in range(size - 1):
        below = row[:, :1] > k
        inverse = 1.0 / a_r[k : k + 1, k : k + 1]
        f_r = jnp.where(below, a_r[:, k : k + 1] * inverse, 0.0)
        f_i = jnp.where(below, a_i[:, k : k + 1] * inverse, 0.0)
        p_r, p_i = a_r[k : k + 1], a_i[k : k + 1]
        q_r, q_i = j_r[k : k + 1], j_i[k : k + 1]
        a_r, a_i = a_r - (f_r * p_r - f_i * p_i), a_i - (f_r * p_i + f_i * p_r)
        j_r, j_i = j_r - (f_r * q_r - f_i * q_i), j_i - (f_r * q_i + f_i * q_r)
    pivots = jnp.sum(jnp.where(row == col, a_r, 0.0), axis=1, keepdims=True)
    scale = 1.0 / jnp.sqrt(pivots)
    j_r, j_i = j_r * scale, j_i * scale
    by_real = jnp.concatenate([j_r, j_i], 0)
    by_imag = jnp.concatenate([-j_i, j_r], 0)
    return lax.dot_general(
        by_real, y_real, (((1,), (0,)), ((), ())), preferred_element_type=f32, precision=highest
    ) + lax.dot_general(
        by_imag, y_imag, (((1,), (0,)), ((), ())), preferred_element_type=f32, precision=highest
    )


def weights_kernel(
    flag, place, voltages, picks, steering, out, v, vt, basis, basis_t, wide, narrow, spread, state, sems
):
    inverse_count = 1.0 / SNAPSHOT_COUNT

    def copy(n, part):
        rows = pl.ds(n * ROWS, ROWS)
        return pltpu.make_async_copy(voltages.at[n, part], v.at[part, rows], sems.at[n, part])

    for n in range(TILES):
        for part in range(2):
            copy(n, part).start()

    squares = jnp.zeros((8, ARRAY_ELEMENTS), f32)
    for n in range(TILES):
        for part in range(2):
            copy(n, part).wait()
            block = v[part, n * ROWS : (n + 1) * ROWS, :]
            vt[part, :, n * ROWS : (n + 1) * ROWS] = block.T
            exact = block.astype(f32)
            squares = squares + jnp.sum((exact * exact).reshape(ROWS // 8, 8, ARRAY_ELEMENTS), axis=0)
    power = jnp.sum(jnp.sum(squares, axis=0, keepdims=True), axis=1, keepdims=True)
    load = diagonal_loading * (power * inverse_count) / ARRAY_ELEMENTS

    for n in range(ARRAY_ELEMENTS // WIDE):
        cols = pl.ds(n * WIDE, WIDE)
        taken_r = plain(picks[...], vt[0, :, cols])
        taken_i = plain(picks[...], vt[1, :, cols])
        wide[: 2 * SUBSPACE_SIZE, cols] = jnp.concatenate([taken_r, -taken_i], 0).astype(bf16)
    spread[...] = through(wide.at[: 2 * SUBSPACE_SIZE], v, 1, 1) * inverse_count
    spread[...] = unit_rows(spread[...])

    def sweep(n, carry):
        wide[...] = pieces(spread[...])
        wide[...] = pieces(through(wide, vt, 3, -1))
        spread[...] = through(wide, v, 3, 1) * inverse_count
        spread[...] = unit_rows(spread[...])
        return carry

    lax.fori_loop(0, SUB_ITERS - 1, sweep, 0)
    found = spread[...] * flag[0].astype(f32)
    blank = jnp.zeros((SUBSPACE_SIZE, ARRAY_ELEMENTS), bf16)
    basis[...] = jnp.concatenate(
        [pieces(found[:SUBSPACE_SIZE]), blank, pieces(found[SUBSPACE_SIZE:]), blank], 0
    )
    basis_t[...] = basis[...].T

    def project(x):
        narrow[...] = pieces(x)
        raw = fold(plain(narrow[...], basis_t[...]), 3)
        half = BEAM_COUNT
        c_r = raw[:half, :128] + raw[half:, 128:]
        c_i = raw[half:, :128] - raw[:half, 128:]
        c = jnp.concatenate([c_r, c_i], 0)
        c = c + pltpu.roll(c, 64, 1)
        c = c + pltpu.roll(c, 32, 1)
        c_split = pieces(c)
        d_split = pieces(jnp.concatenate([-c[half:], c[:half]], 0))
        both = jnp.concatenate([c_split, d_split], 1)
        return x - fold(plain(both, basis[...]), 3)

    source = steering[...]
    state[0] = jnp.zeros_like(source)
    clean = project(source)
    state[1] = clean
    state[2] = clean
    state[3] = source - clean
    inside = beam_sum((source - clean) * (source - clean))

    def correlate():
        narrow[...] = pieces(state[2])
        return through(narrow, vt, 3, -1)

    def curvature_of(seen, direction, tau):
        return beam_sum(seen * seen) * inverse_count + load * (
            beam_sum(direction * direction) + tau * tau * inside
        )

    def iterate(n, carry):
        norm, xi, rho, tau = carry
        seen = correlate()
        direction = state[2]
        step = norm / curvature_of(seen, direction, tau)
        narrow[...] = pieces(seen)
        mapped = project(through(narrow, v, 3, 1) * inverse_count) + load * direction
        state[0] = state[0] + twice(step) * direction
        residual = state[1] - twice(step) * mapped
        state[1] = residual
        xi = xi + step * tau
        rho = rho - step * (load * tau)
        fresh = beam_sum(residual * residual) + rho * rho * inside
        ratio = fresh / norm
        state[2] = residual + twice(ratio) * direction
        tau = rho + ratio * tau
        return fresh, xi, rho, tau

    one = jnp.ones((BEAM_COUNT, 1), f32)
    first = (beam_sum(source * source), jnp.zeros((BEAM_COUNT, 1), f32), one, one)
    norm, xi, rho, tau = lax.fori_loop(0, CG_ITERS - 1, iterate, first)
    direction = state[2]
    step = norm / curvature_of(correlate(), direction, tau)
    solved = state[0] + twice(step) * direction + twice(xi + step * tau) * state[3]
    response = beam_sum(source * solved)
    state[0] = ARRAY_ELEMENTS * solved / twice(response)
    out[...] = state[0, :, pl.ds(pl.multiple_of(place[0] * ROWS, ROWS), ROWS)]


def local_weights(flag, place, gathered, picks, steering, interpret=False):
    vmem = pl.BlockSpec(memory_space=pltpu.VMEM)
    smem = pl.BlockSpec(memory_space=pltpu.SMEM)
    return pl.pallas_call(
        weights_kernel,
        out_shape=jax.ShapeDtypeStruct((2 * BEAM_COUNT, ROWS), f32),
        in_specs=[smem, smem, pl.BlockSpec(memory_space=pl.ANY), vmem, vmem],
        out_specs=vmem,
        scratch_shapes=[
            pltpu.VMEM((2, SNAPSHOT_COUNT, ARRAY_ELEMENTS), bf16),
            pltpu.VMEM((2, ARRAY_ELEMENTS, SNAPSHOT_COUNT), bf16),
            pltpu.VMEM((8 * SUBSPACE_SIZE, ARRAY_ELEMENTS), bf16),
            pltpu.VMEM((ARRAY_ELEMENTS, 8 * SUBSPACE_SIZE), bf16),
            pltpu.VMEM((6 * SUBSPACE_SIZE, ARRAY_ELEMENTS), bf16),
            pltpu.VMEM((6 * BEAM_COUNT, ARRAY_ELEMENTS), bf16),
            pltpu.VMEM((2 * SUBSPACE_SIZE, ARRAY_ELEMENTS), f32),
            pltpu.VMEM((4, 2 * BEAM_COUNT, ARRAY_ELEMENTS), f32),
            pltpu.SemaphoreType.DMA((TILES, 2)),
        ],
        compiler_params=pltpu.CompilerParams(vmem_limit_bytes=58 << 20),
        interpret=interpret,
    )(flag, place, gathered, picks, steering)


def steering_table(beam_entries):
    element_index = jnp.arange(ARRAY_ELEMENTS, dtype=jnp.int32)
    steer_phases = (beam_entries[..., None] * element_index % ARRAY_ELEMENTS).astype(f32) * (
        2.0 * math.pi / ARRAY_ELEMENTS
    )
    return jnp.concatenate([jnp.cos(steer_phases), jnp.sin(steer_phases)], axis=0)


def shards(voltages, rfi_flags, beam_steer_index, start_columns):
    turned = lax.all_to_all(voltages, "chan", split_axis=0, concat_axis=3, tiled=True)
    place = lax.axis_index(TILE)
    gathered = lax.all_gather(turned[0], TILE, axis=0, tiled=False)
    own = lax.dynamic_slice_in_dim(gathered, place * ROWS, ROWS, 3)
    swapped = jnp.stack([own[:, 1], -own[:, 0]], 1)
    real_part = jnp.einsum("tpsi,tpsj->ij", own, gathered, preferred_element_type=f32)
    imag_part = jnp.einsum("tpsi,tpsj->ij", swapped, gathered, preferred_element_type=f32)
    covariance = jnp.stack([real_part, imag_part])[None] * (1.0 / SNAPSHOT_COUNT)
    picks = (start_columns[0][:, None] == jnp.arange(ARRAY_ELEMENTS, dtype=jnp.int32)).astype(bf16)
    steering = steering_table(beam_steer_index[0])
    weights = local_weights(rfi_flags, place[None].astype(jnp.int32), gathered, picks, steering)
    weights = jnp.swapaxes(weights.reshape(1, 2, BEAM_COUNT, ROWS), 1, 2)
    return (covariance, weights)


def solution(mesh):
    split = Mesh(mesh.devices.reshape(mesh.shape["chan"], 4, 4), ("chan", "tile_0", "tile_1"))
    return jax.shard_map(
        shards,
        mesh=split,
        in_specs=(P(None, None, TILE, "chan"), P("chan"), P("chan", None), P("chan", None)),
        out_specs=(P("chan", None, TILE, None), P("chan", None, None, TILE)),
        check_vma=False,
    )
```

```python
import functools
import math

import jax
import jax.numpy as jnp
from jax import lax
from jax.experimental import pallas as pl
from jax.experimental.pallas import tpu as pltpu
from jax.sharding import Mesh
from jax.sharding import PartitionSpec as P

ARRAY_ELEMENTS = 2048
SNAPSHOT_COUNT = 2048
SUBSPACE_SIZE = 32
BEAM_COUNT = 8
SUB_ITERS = 4
CG_ITERS = 12
TILE = ("tile_0", "tile_1")
TILES = 16
ROWS = 128
WIDE = 256
SPLIT = (32, 96)

diagonal_loading = 0.1
f32 = jnp.float32
bf16 = jnp.bfloat16


def pieces(x, count=3):
    terms = [x.astype(bf16)]
    for _ in range(count - 1):
        x = x - terms[-1].astype(f32)
        terms.append(x.astype(bf16))
    return jnp.concatenate(terms, 0)


def fold(x, count):
    rows = x.shape[0] // count
    total = x[:rows]
    for n in range(1, count):
        total = total + x[n * rows : (n + 1) * rows]
    return total


def plain(a, b):
    return lax.dot_general(a, b, (((1,), (0,)), ((), ())), preferred_element_type=f32)


def turned_dot(a, b):
    return lax.dot_general(a, b, (((1,), (1,)), ((), ())), preferred_element_type=f32)


def tile_through(lhs, matrix, cols, count, sign):
    by_real = fold(plain(lhs[...], matrix[0, :, cols]), count)
    by_imag = fold(plain(lhs[...], matrix[1, :, cols]), count)
    half = by_real.shape[0] // 2
    swapped = jnp.concatenate([-by_imag[half:], by_imag[:half]], 0)
    return by_real + swapped if sign > 0 else by_real - swapped


def column_tiles():
    return [pl.ds(n * WIDE, WIDE) for n in range(ARRAY_ELEMENTS // WIDE)]


def beam_sum(x):
    folded = x[:BEAM_COUNT] + x[BEAM_COUNT:]
    return jnp.sum(folded, axis=1, keepdims=True)


def twice(x):
    return jnp.concatenate([x, x], 0)


def every_group(x):
    x = x + pltpu.roll(x, 64, 1)
    return x + pltpu.roll(x, 32, 1)


def stack_pieces(y):
    blank = jnp.zeros((SUBSPACE_SIZE, y.shape[1]), bf16)
    return jnp.concatenate(
        [pieces(y[:SUBSPACE_SIZE]), blank, pieces(y[SUBSPACE_SIZE:]), blank], 0
    )


def unit_rows(stacked, store):
    size = SUBSPACE_SIZE
    raw = turned_dot(stacked[...], stacked[...])
    top, bottom = fold(raw[: 4 * size], 4), fold(raw[4 * size :], 4)
    g_r = every_group(top[:, : 4 * size] + bottom[:, 4 * size :])
    g_i = every_group(bottom[:, : 4 * size] - top[:, 4 * size :])
    row = lax.broadcasted_iota(jnp.int32, (size, 4 * size), 0)
    lane = lax.broadcasted_iota(jnp.int32, (size, 4 * size), 1)
    a_r = jnp.where(lane < size, g_r, jnp.where(lane - size == row, 1.0, 0.0))
    a_i = jnp.where(lane < size, g_i, 0.0)
    blocks = size // 8
    a_r = [a_r[8 * n : 8 * n + 8] for n in range(blocks)]
    a_i = [a_i[8 * n : 8 * n + 8] for n in range(blocks)]
    within = lax.broadcasted_iota(jnp.int32, (8, 1), 0)
    pivots = []
    for k in range(size):
        own, at = k // 8, k % 8
        pivot = a_r[own][at : at + 1, k : k + 1]
        pivots.append(pivot)
        inverse = 1.0 / pivot
        p_r = a_r[own][at : at + 1] * inverse
        p_i = a_i[own][at : at + 1] * inverse
        for n in range((k + 1) // 8, blocks):
            f_r, f_i = a_r[n][:, k : k + 1], a_i[n][:, k : k + 1]
            if n == own:
                f_r = jnp.where(within > at, f_r, 0.0)
                f_i = jnp.where(within > at, f_i, 0.0)
            a_r[n], a_i[n] = (
                a_r[n] - (f_r * p_r - f_i * p_i),
                a_i[n] - (f_r * p_i + f_i * p_r),
            )
    scale = 1.0 / jnp.sqrt(jnp.concatenate(pivots, 0))
    middle = (lane >= size) & (lane < 2 * size)
    j_r = every_group(jnp.where(middle, jnp.concatenate(a_r, 0) * scale, 0.0))
    j_i = every_group(jnp.where(middle, jnp.concatenate(a_i, 0) * scale, 0.0))
    lhs = pieces(
        jnp.concatenate([jnp.concatenate([j_r, -j_i], 1), jnp.concatenate([j_i, j_r], 1)], 0)
    )
    for cols in column_tiles():
        store(cols, fold(plain(lhs, stacked[:, cols]), 3))


def weights_kernel(
    flag, place, early, late, picks, steering, cov_out, out,
    v, vt, basis, basis_t, wide, seen, narrow, cov, state, sems, out_sems,
):
    inverse_count = 1.0 / SNAPSHOT_COUNT
    tiles = column_tiles()
    sources = (early, late)

    def copy(h, n, part):
        rows = pl.ds(TILES * sum(SPLIT[:h]) + n * SPLIT[h], SPLIT[h])
        return pltpu.make_async_copy(sources[h].at[n, part], v.at[part, rows], sems.at[h, n, part])

    for h in range(2):
        for n in range(TILES):
            for part in range(2):
                copy(h, n, part).start()

    squares = jnp.zeros((8, ARRAY_ELEMENTS), f32)
    for h in range(2):
        for group in range(0, TILES, 4):
            for part in range(2):
                for n in range(group, group + 4):
                    copy(h, n, part).wait()
                start = TILES * sum(SPLIT[:h]) + group * SPLIT[h]
                for first in range(start, start + 4 * SPLIT[h], ROWS):
                    block = v[part, first : first + ROWS, :]
                    vt[part, :, first : first + ROWS] = block.T
                    exact = block.astype(f32)
                    squares = squares + jnp.sum(
                        (exact * exact).reshape(ROWS // 8, 8, ARRAY_ELEMENTS), axis=0
                    )
    power = jnp.sum(jnp.sum(squares, axis=0, keepdims=True), axis=1, keepdims=True)
    load = diagonal_loading * (power * inverse_count) / ARRAY_ELEMENTS

    own = pl.ds(pl.multiple_of(place[0] * ROWS, ROWS), ROWS)

    def covariance_tiles(sweep_index):
        for n in range(2):
            cols = pl.ds(pl.multiple_of((2 * sweep_index + n) * WIDE, WIDE), WIDE)
            lhs = jnp.concatenate([vt[0, own, :], vt[1, own, :]], 0)
            by_real, by_imag = plain(lhs, v[0, :, cols]), plain(lhs, v[1, :, cols])
            cov[0, :, cols] = (by_real[:ROWS] + by_imag[ROWS:]) * inverse_count
            cov[1, :, cols] = (by_real[ROWS:] - by_imag[:ROWS]) * inverse_count

    def cov_copy(part):
        return pltpu.make_async_copy(cov.at[part], cov_out.at[part], out_sems.at[part])

    exact_rows = wide.at[: 2 * SUBSPACE_SIZE]
    for cols in tiles:
        taken_r = plain(picks[...], vt[0, :, cols])
        taken_i = plain(picks[...], vt[1, :, cols])
        exact_rows[:, cols] = jnp.concatenate([taken_r, -taken_i], 0).astype(bf16)
    for cols in tiles:
        basis[:, cols] = stack_pieces(tile_through(exact_rows, v, cols, 1, 1) * inverse_count)

    def to_wide(cols, q):
        wide[:, cols] = pieces(q, 2)

    def sweep(n, carry):
        covariance_tiles(n)
        unit_rows(basis, to_wide)
        for cols in tiles:
            seen[:, cols] = pieces(tile_through(wide, vt, cols, 2, -1), 2)
        for cols in tiles:
            basis[:, cols] = stack_pieces(tile_through(seen, v, cols, 2, 1) * inverse_count)
        return carry

    lax.fori_loop(0, SUB_ITERS - 1, sweep, 0)
    covariance_tiles(SUB_ITERS - 1)
    for part in range(2):
        cov_copy(part).start()
    flagged = flag[0].astype(f32)

    def keep(cols, q):
        basis[:, cols] = stack_pieces(q * flagged)
        basis_t[cols, :] = basis[:, cols].T

    unit_rows(basis, keep)

    def coefficients(cols, x):
        return fold(plain(pieces(x), basis_t[cols, :]), 3)

    def remove(raw):
        half = BEAM_COUNT
        c_r = raw[:half, :128] + raw[half:, 128:]
        c_i = raw[half:, :128] - raw[:half, 128:]
        c = every_group(jnp.concatenate([c_r, c_i], 0))
        crossed = jnp.concatenate([-c[half:], c[:half]], 0)
        both = pieces(jnp.concatenate([c, crossed], 1))
        return jnp.concatenate([fold(plain(both, basis[:, cols]), 3) for cols in tiles], 1)

    source = steering[...]
    state[0] = jnp.zeros_like(source)
    held = remove(sum(coefficients(cols, steering[:, cols]) for cols in tiles))
    clean = source - held
    state[1] = clean
    state[2] = clean
    state[3] = held
    inside = beam_sum(held * held)

    def correlate(write):
        narrow[...] = pieces(state[2])
        total = jnp.zeros((2 * BEAM_COUNT, WIDE), f32)
        for cols in tiles:
            part = tile_through(narrow, vt, cols, 3, -1)
            if write:
                seen[: 6 * BEAM_COUNT, cols] = pieces(part)
            total = total + part * part
        return beam_sum(total)

    def curvature_of(energy, direction, tau):
        return energy * inverse_count + load * (
            beam_sum(direction * direction) + tau * tau * inside
        )

    def iterate(n, carry):
        norm, xi, rho, tau = carry
        energy = correlate(True)
        direction = state[2]
        step = norm / curvature_of(energy, direction, tau)
        state[0] = state[0] + twice(step) * direction
        state[1] = state[1] - twice(step * load) * direction
        xi = xi + step * tau
        rho = rho - step * (load * tau)
        raw = jnp.zeros((2 * BEAM_COUNT, WIDE), f32)
        for cols in tiles:
            mapped = tile_through(seen.at[: 6 * BEAM_COUNT], v, cols, 3, 1) * inverse_count
            raw = raw + coefficients(cols, mapped)
            state[4, :, cols] = mapped
        residual = state[1] - twice(step) * (state[4] - remove(raw))
        state[1] = residual
        fresh = beam_sum(residual * residual) + rho * rho * inside
        ratio = fresh / norm
        state[2] = residual + twice(ratio) * direction
        tau = rho + ratio * tau
        return fresh, xi, rho, tau

    one = jnp.ones((BEAM_COUNT, 1), f32)
    first = (beam_sum(source * source), jnp.zeros((BEAM_COUNT, 1), f32), one, one)
    norm, xi, rho, tau = lax.fori_loop(0, CG_ITERS - 1, iterate, first)
    direction = state[2]
    step = norm / curvature_of(correlate(False), direction, tau)
    solved = state[0] + twice(step) * direction + twice(xi + step * tau) * state[3]
    response = beam_sum(source * solved)
    state[0] = ARRAY_ELEMENTS * solved / twice(response)
    out[...] = state[0, :, own]
    for part in range(2):
        cov_copy(part).wait()


def local_weights(flag, place, early, late, picks, steering, interpret=False):
    vmem = pl.BlockSpec(memory_space=pltpu.VMEM)
    smem = pl.BlockSpec(memory_space=pltpu.SMEM)
    hbm = pl.BlockSpec(memory_space=pl.ANY)
    return pl.pallas_call(
        weights_kernel,
        out_shape=(
            jax.ShapeDtypeStruct((2, ROWS, ARRAY_ELEMENTS), f32),
            jax.ShapeDtypeStruct((2 * BEAM_COUNT, ROWS), f32),
        ),
        in_specs=[smem, smem, hbm, hbm, vmem, vmem],
        out_specs=(hbm, vmem),
        scratch_shapes=[
            pltpu.VMEM((2, SNAPSHOT_COUNT, ARRAY_ELEMENTS), bf16),
            pltpu.VMEM((2, ARRAY_ELEMENTS, SNAPSHOT_COUNT), bf16),
            pltpu.VMEM((8 * SUBSPACE_SIZE, ARRAY_ELEMENTS), bf16),
            pltpu.VMEM((ARRAY_ELEMENTS, 8 * SUBSPACE_SIZE), bf16),
            pltpu.VMEM((4 * SUBSPACE_SIZE, ARRAY_ELEMENTS), bf16),
            pltpu.VMEM((4 * SUBSPACE_SIZE, SNAPSHOT_COUNT), bf16),
            pltpu.VMEM((6 * BEAM_COUNT, ARRAY_ELEMENTS), bf16),
            pltpu.VMEM((2, ROWS, ARRAY_ELEMENTS), f32),
            pltpu.VMEM((5, 2 * BEAM_COUNT, ARRAY_ELEMENTS), f32),
            pltpu.SemaphoreType.DMA((2, TILES, 2)),
            pltpu.SemaphoreType.DMA((2,)),
        ],
        compiler_params=pltpu.CompilerParams(vmem_limit_bytes=58 << 20),
        interpret=interpret,
    )(flag, place, early, late, picks, steering)


def steering_table(beam_entries):
    element_index = jnp.arange(ARRAY_ELEMENTS, dtype=jnp.int32)
    steer_phases = (beam_entries[..., None] * element_index % ARRAY_ELEMENTS).astype(f32) * (
        2.0 * math.pi / ARRAY_ELEMENTS
    )
    return jnp.concatenate([jnp.cos(steer_phases), jnp.sin(steer_phases)], axis=0)


def shards(voltages, rfi_flags, beam_steer_index, start_columns):
    place = lax.axis_index(TILE)
    gathered = []
    for first, rows in zip((0, SPLIT[0]), SPLIT):
        turned = lax.all_to_all(
            voltages[:, :, first : first + rows], "chan", split_axis=0, concat_axis=3, tiled=True
        )
        gathered.append(lax.all_gather(turned[0], TILE, axis=0, tiled=False))
    picks = (start_columns[0][:, None] == jnp.arange(ARRAY_ELEMENTS, dtype=jnp.int32)).astype(bf16)
    steering = steering_table(beam_steer_index[0])
    covariance, weights = local_weights(
        rfi_flags, place[None].astype(jnp.int32), *gathered, picks, steering
    )
    weights = jnp.swapaxes(weights.reshape(1, 2, BEAM_COUNT, ROWS), 1, 2)
    return (covariance[None], weights)


def solution(mesh):
    split = Mesh(mesh.devices.reshape(mesh.shape["chan"], 4, 4), ("chan", "tile_0", "tile_1"))
    return jax.shard_map(
        shards,
        mesh=split,
        in_specs=(P(None, None, TILE, "chan"), P("chan"), P("chan", None), P("chan", None)),
        out_specs=(P("chan", None, TILE, None), P("chan", None, None, TILE)),
        check_vma=False,
    )
```

```python
import functools
import math

import jax
import jax.numpy as jnp
from jax import lax
from jax.experimental import pallas as pl
from jax.experimental.pallas import tpu as pltpu
from jax.sharding import Mesh
from jax.sharding import PartitionSpec as P

ARRAY_ELEMENTS = 2048
SNAPSHOT_COUNT = 2048
SUBSPACE_SIZE = 32
BEAM_COUNT = 8
SUB_ITERS = 4
CG_ITERS = 12
TILE = ("tile_0", "tile_1")
TILES = 16
ROWS = 128
WIDE = 256

diagonal_loading = 0.1
f32 = jnp.float32
bf16 = jnp.bfloat16


def pieces(x, count=3):
    terms = [x.astype(bf16)]
    for _ in range(count - 1):
        x = x - terms[-1].astype(f32)
        terms.append(x.astype(bf16))
    return jnp.concatenate(terms, 0)


def fold(x, count):
    rows = x.shape[0] // count
    total = x[:rows]
    for n in range(1, count):
        total = total + x[n * rows : (n + 1) * rows]
    return total


def plain(a, b):
    return lax.dot_general(a, b, (((1,), (0,)), ((), ())), preferred_element_type=f32)


def turned_dot(a, b):
    return lax.dot_general(a, b, (((1,), (1,)), ((), ())), preferred_element_type=f32)


def tile_through(lhs, matrix, cols, count, sign):
    by_real = fold(plain(lhs[...], matrix[0, :, cols]), count)
    by_imag = fold(plain(lhs[...], matrix[1, :, cols]), count)
    half = by_real.shape[0] // 2
    swapped = jnp.concatenate([-by_imag[half:], by_imag[:half]], 0)
    return by_real + swapped if sign > 0 else by_real - swapped


def column_tiles():
    return [pl.ds(n * WIDE, WIDE) for n in range(ARRAY_ELEMENTS // WIDE)]


def beam_sum(x):
    folded = x[:BEAM_COUNT] + x[BEAM_COUNT:]
    return jnp.sum(folded, axis=1, keepdims=True)


def twice(x):
    return jnp.concatenate([x, x], 0)


def every_group(x):
    x = x + pltpu.roll(x, 64, 1)
    return x + pltpu.roll(x, 32, 1)


def stack_pieces(y):
    blank = jnp.zeros((SUBSPACE_SIZE, y.shape[1]), bf16)
    return jnp.concatenate(
        [pieces(y[:SUBSPACE_SIZE]), blank, pieces(y[SUBSPACE_SIZE:]), blank], 0
    )


def unit_rows(stacked, store):
    size = SUBSPACE_SIZE
    raw = turned_dot(stacked[...], stacked[...])
    top, bottom = fold(raw[: 4 * size], 4), fold(raw[4 * size :], 4)
    g_r = every_group(top[:, : 4 * size] + bottom[:, 4 * size :])
    g_i = every_group(bottom[:, : 4 * size] - top[:, 4 * size :])
    row = lax.broadcasted_iota(jnp.int32, (size, 4 * size), 0)
    lane = lax.broadcasted_iota(jnp.int32, (size, 4 * size), 1)
    a_r = jnp.where(lane < size, g_r, jnp.where(lane - size == row, 1.0, 0.0))
    a_i = jnp.where(lane < size, g_i, 0.0)
    blocks = size // 8
    a_r = [a_r[8 * n : 8 * n + 8] for n in range(blocks)]
    a_i = [a_i[8 * n : 8 * n + 8] for n in range(blocks)]
    within = lax.broadcasted_iota(jnp.int32, (8, 1), 0)
    pivots = []
    for k in range(size):
        own, at = k // 8, k % 8
        pivot = a_r[own][at : at + 1, k : k + 1]
        pivots.append(pivot)
        inverse = 1.0 / pivot
        p_r = a_r[own][at : at + 1] * inverse
        p_i = a_i[own][at : at + 1] * inverse
        for n in range((k + 1) // 8, blocks):
            f_r, f_i = a_r[n][:, k : k + 1], a_i[n][:, k : k + 1]
            if n == own:
                f_r = jnp.where(within > at, f_r, 0.0)
                f_i = jnp.where(within > at, f_i, 0.0)
            a_r[n], a_i[n] = (
                a_r[n] - (f_r * p_r - f_i * p_i),
                a_i[n] - (f_r * p_i + f_i * p_r),
            )
    scale = 1.0 / jnp.sqrt(jnp.concatenate(pivots, 0))
    middle = (lane >= size) & (lane < 2 * size)
    j_r = every_group(jnp.where(middle, jnp.concatenate(a_r, 0) * scale, 0.0))
    j_i = every_group(jnp.where(middle, jnp.concatenate(a_i, 0) * scale, 0.0))
    lhs = pieces(
        jnp.concatenate([jnp.concatenate([j_r, -j_i], 1), jnp.concatenate([j_i, j_r], 1)], 0)
    )
    for cols in column_tiles():
        store(cols, fold(plain(lhs, stacked[:, cols]), 3))


def weights_kernel(
    flag, place, gathered, picks, steering, cov_out, out,
    v, vt, basis, basis_t, wide, seen, narrow, cov, state, sems, out_sems,
):
    inverse_count = 1.0 / SNAPSHOT_COUNT
    tiles = column_tiles()

    def copy(n, part):
        rows = pl.ds(n * ROWS, ROWS)
        return pltpu.make_async_copy(gathered.at[n, part], v.at[part, rows], sems.at[n, part])

    for n in range(TILES):
        for part in range(2):
            copy(n, part).start()

    squares = jnp.zeros((8, ARRAY_ELEMENTS), f32)
    for n in range(TILES):
        for part in range(2):
            copy(n, part).wait()
            block = v[part, n * ROWS : (n + 1) * ROWS, :]
            vt[part, :, n * ROWS : (n + 1) * ROWS] = block.T
            exact = block.astype(f32)
            squares = squares + jnp.sum((exact * exact).reshape(ROWS // 8, 8, ARRAY_ELEMENTS), axis=0)
    power = jnp.sum(jnp.sum(squares, axis=0, keepdims=True), axis=1, keepdims=True)
    load = diagonal_loading * (power * inverse_count) / ARRAY_ELEMENTS

    own = pl.ds(pl.multiple_of(place[0] * ROWS, ROWS), ROWS)

    def covariance_tiles(sweep_index):
        for n in range(2):
            cols = pl.ds(pl.multiple_of((2 * sweep_index + n) * WIDE, WIDE), WIDE)
            lhs = jnp.concatenate([vt[0, own, :], vt[1, own, :]], 0)
            by_real, by_imag = plain(lhs, v[0, :, cols]), plain(lhs, v[1, :, cols])
            cov[0, :, cols] = (by_real[:ROWS] + by_imag[ROWS:]) * inverse_count
            cov[1, :, cols] = (by_real[ROWS:] - by_imag[:ROWS]) * inverse_count

    def cov_copy(part):
        return pltpu.make_async_copy(cov.at[part], cov_out.at[part], out_sems.at[part])

    exact_rows = wide.at[: 2 * SUBSPACE_SIZE]
    for cols in tiles:
        taken_r = plain(picks[...], vt[0, :, cols])
        taken_i = plain(picks[...], vt[1, :, cols])
        exact_rows[:, cols] = jnp.concatenate([taken_r, -taken_i], 0).astype(bf16)
    for cols in tiles:
        basis[:, cols] = stack_pieces(tile_through(exact_rows, v, cols, 1, 1) * inverse_count)

    def to_wide(cols, q):
        wide[:, cols] = pieces(q, 2)

    def sweep(n, carry):
        covariance_tiles(n)
        unit_rows(basis, to_wide)
        for cols in tiles:
            seen[:, cols] = pieces(tile_through(wide, vt, cols, 2, -1), 2)
        for cols in tiles:
            basis[:, cols] = stack_pieces(tile_through(seen, v, cols, 2, 1) * inverse_count)
        return carry

    lax.fori_loop(0, SUB_ITERS - 1, sweep, 0)
    covariance_tiles(SUB_ITERS - 1)
    for part in range(2):
        cov_copy(part).start()
    flagged = flag[0].astype(f32)

    def keep(cols, q):
        basis[:, cols] = stack_pieces(q * flagged)
        basis_t[cols, :] = basis[:, cols].T

    unit_rows(basis, keep)

    def coefficients(cols, x):
        return fold(plain(pieces(x), basis_t[cols, :]), 3)

    def remove(raw):
        half = BEAM_COUNT
        c_r = raw[:half, :128] + raw[half:, 128:]
        c_i = raw[half:, :128] - raw[:half, 128:]
        c = every_group(jnp.concatenate([c_r, c_i], 0))
        crossed = jnp.concatenate([-c[half:], c[:half]], 0)
        both = pieces(jnp.concatenate([c, crossed], 1))
        return jnp.concatenate([fold(plain(both, basis[:, cols]), 3) for cols in tiles], 1)

    source = steering[...]
    state[0] = jnp.zeros_like(source)
    held = remove(sum(coefficients(cols, steering[:, cols]) for cols in tiles))
    clean = source - held
    state[1] = clean
    state[2] = clean
    state[3] = held
    inside = beam_sum(held * held)

    def correlate(write):
        narrow[...] = pieces(state[2])
        total = jnp.zeros((2 * BEAM_COUNT, WIDE), f32)
        for cols in tiles:
            part = tile_through(narrow, vt, cols, 3, -1)
            if write:
                seen[: 6 * BEAM_COUNT, cols] = pieces(part)
            total = total + part * part
        return beam_sum(total)

    def curvature_of(energy, direction, tau):
        return energy * inverse_count + load * (
            beam_sum(direction * direction) + tau * tau * inside
        )

    def iterate(n, carry):
        norm, xi, rho, tau = carry
        energy = correlate(True)
        direction = state[2]
        step = norm / curvature_of(energy, direction, tau)
        state[0] = state[0] + twice(step) * direction
        state[1] = state[1] - twice(step * load) * direction
        xi = xi + step * tau
        rho = rho - step * (load * tau)
        raw = jnp.zeros((2 * BEAM_COUNT, WIDE), f32)
        for cols in tiles:
            mapped = tile_through(seen.at[: 6 * BEAM_COUNT], v, cols, 3, 1) * inverse_count
            raw = raw + coefficients(cols, mapped)
            state[4, :, cols] = mapped
        residual = state[1] - twice(step) * (state[4] - remove(raw))
        state[1] = residual
        fresh = beam_sum(residual * residual) + rho * rho * inside
        ratio = fresh / norm
        state[2] = residual + twice(ratio) * direction
        tau = rho + ratio * tau
        return fresh, xi, rho, tau

    one = jnp.ones((BEAM_COUNT, 1), f32)
    first = (beam_sum(source * source), jnp.zeros((BEAM_COUNT, 1), f32), one, one)
    norm, xi, rho, tau = lax.fori_loop(0, CG_ITERS - 1, iterate, first)
    direction = state[2]
    step = norm / curvature_of(correlate(False), direction, tau)
    solved = state[0] + twice(step) * direction + twice(xi + step * tau) * state[3]
    response = beam_sum(source * solved)
    state[0] = ARRAY_ELEMENTS * solved / twice(response)
    out[...] = state[0, :, own]
    for part in range(2):
        cov_copy(part).wait()


def local_weights(flag, place, gathered, picks, steering, interpret=False):
    vmem = pl.BlockSpec(memory_space=pltpu.VMEM)
    smem = pl.BlockSpec(memory_space=pltpu.SMEM)
    hbm = pl.BlockSpec(memory_space=pl.ANY)
    return pl.pallas_call(
        weights_kernel,
        out_shape=(
            jax.ShapeDtypeStruct((2, ROWS, ARRAY_ELEMENTS), f32),
            jax.ShapeDtypeStruct((2 * BEAM_COUNT, ROWS), f32),
        ),
        in_specs=[smem, smem, hbm, vmem, vmem],
        out_specs=(hbm, vmem),
        scratch_shapes=[
            pltpu.VMEM((2, SNAPSHOT_COUNT, ARRAY_ELEMENTS), bf16),
            pltpu.VMEM((2, ARRAY_ELEMENTS, SNAPSHOT_COUNT), bf16),
            pltpu.VMEM((8 * SUBSPACE_SIZE, ARRAY_ELEMENTS), bf16),
            pltpu.VMEM((ARRAY_ELEMENTS, 8 * SUBSPACE_SIZE), bf16),
            pltpu.VMEM((4 * SUBSPACE_SIZE, ARRAY_ELEMENTS), bf16),
            pltpu.VMEM((4 * SUBSPACE_SIZE, SNAPSHOT_COUNT), bf16),
            pltpu.VMEM((6 * BEAM_COUNT, ARRAY_ELEMENTS), bf16),
            pltpu.VMEM((2, ROWS, ARRAY_ELEMENTS), f32),
            pltpu.VMEM((5, 2 * BEAM_COUNT, ARRAY_ELEMENTS), f32),
            pltpu.SemaphoreType.DMA((TILES, 2)),
            pltpu.SemaphoreType.DMA((2,)),
        ],
        compiler_params=pltpu.CompilerParams(vmem_limit_bytes=58 << 20),
        interpret=interpret,
    )(flag, place, gathered, picks, steering)


def steering_table(beam_entries):
    element_index = jnp.arange(ARRAY_ELEMENTS, dtype=jnp.int32)
    steer_phases = (beam_entries[..., None] * element_index % ARRAY_ELEMENTS).astype(f32) * (
        2.0 * math.pi / ARRAY_ELEMENTS
    )
    return jnp.concatenate([jnp.cos(steer_phases), jnp.sin(steer_phases)], axis=0)


def shards(voltages, rfi_flags, beam_steer_index, start_columns):
    place = lax.axis_index(TILE)
    turned = lax.all_to_all(voltages, "chan", split_axis=0, concat_axis=3, tiled=True)
    gathered = lax.all_gather(turned[0], TILE, axis=0, tiled=False)
    picks = (start_columns[0][:, None] == jnp.arange(ARRAY_ELEMENTS, dtype=jnp.int32)).astype(bf16)
    steering = steering_table(beam_steer_index[0])
    covariance, weights = local_weights(
        rfi_flags, place[None].astype(jnp.int32), gathered, picks, steering
    )
    weights = jnp.swapaxes(weights.reshape(1, 2, BEAM_COUNT, ROWS), 1, 2)
    return (covariance[None], weights)


def solution(mesh):
    split = Mesh(mesh.devices.reshape(mesh.shape["chan"], 4, 4), ("chan", "tile_0", "tile_1"))
    return jax.shard_map(
        shards,
        mesh=split,
        in_specs=(P(None, None, TILE, "chan"), P("chan"), P("chan", None), P("chan", None)),
        out_specs=(P("chan", None, TILE, None), P("chan", None, None, TILE)),
        check_vma=False,
    )
```

```python
import functools
import math

import jax
import jax.numpy as jnp
from jax import lax
from jax.experimental import pallas as pl
from jax.experimental.pallas import tpu as pltpu
from jax.sharding import Mesh
from jax.sharding import PartitionSpec as P

ARRAY_ELEMENTS = 2048
SNAPSHOT_COUNT = 2048
SUBSPACE_SIZE = 32
BEAM_COUNT = 8
SUB_ITERS = 4
CG_ITERS = 12
TILE = ("tile_0", "tile_1")
TILES = 16
ROWS = 128
WIDE = 256


diagonal_loading = 0.1
f32 = jnp.float32
bf16 = jnp.bfloat16


def pieces(x, count=3):
    terms = [x.astype(bf16)]
    for _ in range(count - 1):
        x = x - terms[-1].astype(f32)
        terms.append(x.astype(bf16))
    return jnp.concatenate(terms, 0)


def fold(x, count):
    rows = x.shape[0] // count
    total = x[:rows]
    for n in range(1, count):
        total = total + x[n * rows : (n + 1) * rows]
    return total


def plain(a, b):
    return lax.dot_general(a, b, (((1,), (0,)), ((), ())), preferred_element_type=f32)


def turned_dot(a, b):
    return lax.dot_general(a, b, (((1,), (1,)), ((), ())), preferred_element_type=f32)


def tile_through(lhs, matrix, cols, count, sign):
    by_real = fold(plain(lhs[...], matrix[0, :, cols]), count)
    by_imag = fold(plain(lhs[...], matrix[1, :, cols]), count)
    half = by_real.shape[0] // 2
    swapped = jnp.concatenate([-by_imag[half:], by_imag[:half]], 0)
    return by_real + swapped if sign > 0 else by_real - swapped


def column_tiles():
    return [pl.ds(n * WIDE, WIDE) for n in range(ARRAY_ELEMENTS // WIDE)]


def beam_sum(x):
    folded = x[:BEAM_COUNT] + x[BEAM_COUNT:]
    return jnp.sum(folded, axis=1, keepdims=True)


def twice(x):
    return jnp.concatenate([x, x], 0)


def every_group(x):
    x = x + pltpu.roll(x, 64, 1)
    return x + pltpu.roll(x, 32, 1)


def stack_pieces(y):
    blank = jnp.zeros((SUBSPACE_SIZE, y.shape[1]), bf16)
    return jnp.concatenate(
        [pieces(y[:SUBSPACE_SIZE]), blank, pieces(y[SUBSPACE_SIZE:]), blank], 0
    )


def unit_rows(stacked, store):
    size = SUBSPACE_SIZE
    raw = turned_dot(stacked[...], stacked[...])
    top, bottom = fold(raw[: 4 * size], 4), fold(raw[4 * size :], 4)
    g_r = every_group(top[:, : 4 * size] + bottom[:, 4 * size :])
    g_i = every_group(bottom[:, : 4 * size] - top[:, 4 * size :])
    row = lax.broadcasted_iota(jnp.int32, (size, 4 * size), 0)
    lane = lax.broadcasted_iota(jnp.int32, (size, 4 * size), 1)
    a_r = jnp.where(lane < size, g_r, jnp.where(lane - size == row, 1.0, 0.0))
    a_i = jnp.where(lane < size, g_i, 0.0)
    blocks = size // 8
    a_r = [a_r[8 * n : 8 * n + 8] for n in range(blocks)]
    a_i = [a_i[8 * n : 8 * n + 8] for n in range(blocks)]
    within = lax.broadcasted_iota(jnp.int32, (8, 1), 0)
    pivots = []
    for k in range(size):
        own, at = k // 8, k % 8
        pivot = a_r[own][at : at + 1, k : k + 1]
        pivots.append(pivot)
        inverse = 1.0 / pivot
        p_r = a_r[own][at : at + 1] * inverse
        p_i = a_i[own][at : at + 1] * inverse
        for n in range((k + 1) // 8, blocks):
            f_r, f_i = a_r[n][:, k : k + 1], a_i[n][:, k : k + 1]
            if n == own:
                f_r = jnp.where(within > at, f_r, 0.0)
                f_i = jnp.where(within > at, f_i, 0.0)
            a_r[n], a_i[n] = (
                a_r[n] - (f_r * p_r - f_i * p_i),
                a_i[n] - (f_r * p_i + f_i * p_r),
            )
    scale = 1.0 / jnp.sqrt(jnp.concatenate(pivots, 0))
    middle = (lane >= size) & (lane < 2 * size)
    j_r = every_group(jnp.where(middle, jnp.concatenate(a_r, 0) * scale, 0.0))
    j_i = every_group(jnp.where(middle, jnp.concatenate(a_i, 0) * scale, 0.0))
    lhs = pieces(
        jnp.concatenate([jnp.concatenate([j_r, -j_i], 1), jnp.concatenate([j_i, j_r], 1)], 0)
    )
    for cols in column_tiles():
        store(cols, fold(plain(lhs, stacked[:, cols]), 3))


def weights_kernel(flag, place, picks, steering, *refs):
    gathered = refs[:TILES]
    cov_out, out = refs[TILES : TILES + 2]
    v, vt, basis, basis_t, wide, seen, narrow, cov, state, sems, out_sems = refs[TILES + 2 :]
    inverse_count = 1.0 / SNAPSHOT_COUNT
    tiles = column_tiles()

    def copy(block, part):
        outer, inner = block // 4, block % 4
        if part == 0:
            piece, half = gathered[2 * outer + inner // 2], inner % 2
        else:
            piece, half = gathered[8 + 2 * inner + outer // 2], outer % 2
        return pltpu.make_async_copy(
            piece.at[pl.ds(half * ROWS, ROWS)], v.at[part, pl.ds(block * ROWS, ROWS)], sems.at[block, part]
        )

    for n in range(TILES):
        for part in range(2):
            copy(n, part).start()

    squares = jnp.zeros((8, ARRAY_ELEMENTS), f32)
    for n in range(TILES):
        for part in range(2):
            copy(n, part).wait()
            block = v[part, n * ROWS : (n + 1) * ROWS, :]
            vt[part, :, n * ROWS : (n + 1) * ROWS] = block.T
            exact = block.astype(f32)
            squares = squares + jnp.sum((exact * exact).reshape(ROWS // 8, 8, ARRAY_ELEMENTS), axis=0)
    power = jnp.sum(jnp.sum(squares, axis=0, keepdims=True), axis=1, keepdims=True)
    load = diagonal_loading * (power * inverse_count) / ARRAY_ELEMENTS

    own = pl.ds(pl.multiple_of(place[0] * ROWS, ROWS), ROWS)

    def covariance_tiles(sweep_index):
        for n in range(2):
            cols = pl.ds(pl.multiple_of((2 * sweep_index + n) * WIDE, WIDE), WIDE)
            lhs = jnp.concatenate([vt[0, own, :], vt[1, own, :]], 0)
            by_real, by_imag = plain(lhs, v[0, :, cols]), plain(lhs, v[1, :, cols])
            cov[0, :, cols] = (by_real[:ROWS] + by_imag[ROWS:]) * inverse_count
            cov[1, :, cols] = (by_real[ROWS:] - by_imag[:ROWS]) * inverse_count

    def cov_copy(part):
        return pltpu.make_async_copy(cov.at[part], cov_out.at[part], out_sems.at[part])

    exact_rows = wide.at[: 2 * SUBSPACE_SIZE]
    for cols in tiles:
        taken_r = plain(picks[...], vt[0, :, cols])
        taken_i = plain(picks[...], vt[1, :, cols])
        exact_rows[:, cols] = jnp.concatenate([taken_r, -taken_i], 0).astype(bf16)
    for cols in tiles:
        basis[:, cols] = stack_pieces(tile_through(exact_rows, v, cols, 1, 1) * inverse_count)

    def to_wide(cols, q):
        wide[:, cols] = pieces(q, 2)

    def sweep(n, carry):
        covariance_tiles(n)
        unit_rows(basis, to_wide)
        for cols in tiles:
            seen[:, cols] = pieces(tile_through(wide, vt, cols, 2, -1), 2)
        for cols in tiles:
            basis[:, cols] = stack_pieces(tile_through(seen, v, cols, 2, 1) * inverse_count)
        return carry

    lax.fori_loop(0, SUB_ITERS - 1, sweep, 0)
    covariance_tiles(SUB_ITERS - 1)
    for part in range(2):
        cov_copy(part).start()
    flagged = flag[0].astype(f32)

    def keep(cols, q):
        basis[:, cols] = stack_pieces(q * flagged)
        basis_t[cols, :] = basis[:, cols].T

    unit_rows(basis, keep)

    def coefficients(cols, x):
        return fold(plain(pieces(x), basis_t[cols, :]), 3)

    def remove(raw):
        half = BEAM_COUNT
        c_r = raw[:half, :128] + raw[half:, 128:]
        c_i = raw[half:, :128] - raw[:half, 128:]
        c = every_group(jnp.concatenate([c_r, c_i], 0))
        crossed = jnp.concatenate([-c[half:], c[:half]], 0)
        both = pieces(jnp.concatenate([c, crossed], 1))
        return jnp.concatenate([fold(plain(both, basis[:, cols]), 3) for cols in tiles], 1)

    source = steering[...]
    state[0] = jnp.zeros_like(source)
    held = remove(sum(coefficients(cols, steering[:, cols]) for cols in tiles))
    clean = source - held
    state[1] = clean
    state[2] = clean
    state[3] = held
    inside = beam_sum(held * held)

    def correlate(write):
        narrow[...] = pieces(state[2])
        total = jnp.zeros((2 * BEAM_COUNT, WIDE), f32)
        for cols in tiles:
            part = tile_through(narrow, vt, cols, 3, -1)
            if write:
                seen[: 6 * BEAM_COUNT, cols] = pieces(part)
            total = total + part * part
        return beam_sum(total)

    def curvature_of(energy, direction, tau):
        return energy * inverse_count + load * (
            beam_sum(direction * direction) + tau * tau * inside
        )

    def iterate(n, carry):
        norm, xi, rho, tau = carry
        energy = correlate(True)
        direction = state[2]
        step = norm / curvature_of(energy, direction, tau)
        state[0] = state[0] + twice(step) * direction
        state[1] = state[1] - twice(step * load) * direction
        xi = xi + step * tau
        rho = rho - step * (load * tau)
        raw = jnp.zeros((2 * BEAM_COUNT, WIDE), f32)
        for cols in tiles:
            mapped = tile_through(seen.at[: 6 * BEAM_COUNT], v, cols, 3, 1) * inverse_count
            raw = raw + coefficients(cols, mapped)
            state[4, :, cols] = mapped
        residual = state[1] - twice(step) * (state[4] - remove(raw))
        state[1] = residual
        fresh = beam_sum(residual * residual) + rho * rho * inside
        ratio = fresh / norm
        state[2] = residual + twice(ratio) * direction
        tau = rho + ratio * tau
        return fresh, xi, rho, tau

    one = jnp.ones((BEAM_COUNT, 1), f32)
    first = (beam_sum(source * source), jnp.zeros((BEAM_COUNT, 1), f32), one, one)
    norm, xi, rho, tau = lax.fori_loop(0, CG_ITERS - 1, iterate, first)
    direction = state[2]
    step = norm / curvature_of(correlate(False), direction, tau)
    solved = state[0] + twice(step) * direction + twice(xi + step * tau) * state[3]
    response = beam_sum(source * solved)
    state[0] = ARRAY_ELEMENTS * solved / twice(response)
    out[...] = state[0, :, own]
    for part in range(2):
        cov_copy(part).wait()


def local_weights(flag, place, gathered, picks, steering, interpret=False):
    vmem = pl.BlockSpec(memory_space=pltpu.VMEM)
    smem = pl.BlockSpec(memory_space=pltpu.SMEM)
    hbm = pl.BlockSpec(memory_space=pl.ANY)
    return pl.pallas_call(
        weights_kernel,
        out_shape=(
            jax.ShapeDtypeStruct((2, ROWS, ARRAY_ELEMENTS), f32),
            jax.ShapeDtypeStruct((2 * BEAM_COUNT, ROWS), f32),
        ),
        in_specs=[smem, smem, vmem, vmem] + [hbm] * TILES,
        out_specs=(hbm, vmem),
        scratch_shapes=[
            pltpu.VMEM((2, SNAPSHOT_COUNT, ARRAY_ELEMENTS), bf16),
            pltpu.VMEM((2, ARRAY_ELEMENTS, SNAPSHOT_COUNT), bf16),
            pltpu.VMEM((8 * SUBSPACE_SIZE, ARRAY_ELEMENTS), bf16),
            pltpu.VMEM((ARRAY_ELEMENTS, 8 * SUBSPACE_SIZE), bf16),
            pltpu.VMEM((4 * SUBSPACE_SIZE, ARRAY_ELEMENTS), bf16),
            pltpu.VMEM((4 * SUBSPACE_SIZE, SNAPSHOT_COUNT), bf16),
            pltpu.VMEM((6 * BEAM_COUNT, ARRAY_ELEMENTS), bf16),
            pltpu.VMEM((2, ROWS, ARRAY_ELEMENTS), f32),
            pltpu.VMEM((5, 2 * BEAM_COUNT, ARRAY_ELEMENTS), f32),
            pltpu.SemaphoreType.DMA((TILES, 2)),
            pltpu.SemaphoreType.DMA((2,)),
        ],
        compiler_params=pltpu.CompilerParams(vmem_limit_bytes=58 << 20),
        interpret=interpret,
    )(flag, place, picks, steering, *gathered)


def ring_gather(block, first, second):
    onward = [(n, (n + 1) % 4) for n in range(4)]
    back = [(n, (n - 1) % 4) for n in range(4)]
    half = block.shape[0] // 2
    before = lax.ppermute(block, first, onward)
    after = lax.ppermute(block, first, back)
    across = (
        lax.ppermute(before[:half], first, onward),
        lax.ppermute(after[half:], first, back),
    )
    near = jnp.concatenate([block, before], 0)
    far = jnp.concatenate([after, *across], 0)
    near_before = lax.ppermute(near, second, onward)
    near_after = lax.ppermute(near, second, back)
    far_before = lax.ppermute(far, second, onward)
    far_after = lax.ppermute(far, second, back)
    near_across = lax.ppermute(near_before, second, onward)
    far_across = lax.ppermute(far_after, second, back)
    return [near, far, near_before, far_before, near_after, far_after, near_across, far_across]


def steering_table(beam_entries):
    element_index = jnp.arange(ARRAY_ELEMENTS, dtype=jnp.int32)
    steer_phases = (beam_entries[..., None] * element_index % ARRAY_ELEMENTS).astype(f32) * (
        2.0 * math.pi / ARRAY_ELEMENTS
    )
    return jnp.concatenate([jnp.cos(steer_phases), jnp.sin(steer_phases)], axis=0)


def shards(voltages, rfi_flags, beam_steer_index, start_columns):
    place = lax.axis_index(TILE)
    turned = lax.all_to_all(voltages, "chan", split_axis=0, concat_axis=3, tiled=True)
    gathered = ring_gather(turned[0, 0], "tile_1", "tile_0")
    gathered += ring_gather(turned[0, 1], "tile_0", "tile_1")
    picks = (start_columns[0][:, None] == jnp.arange(ARRAY_ELEMENTS, dtype=jnp.int32)).astype(bf16)
    steering = steering_table(beam_steer_index[0])
    covariance, weights = local_weights(
        rfi_flags, place[None].astype(jnp.int32), gathered, picks, steering
    )
    weights = jnp.swapaxes(weights.reshape(1, 2, BEAM_COUNT, ROWS), 1, 2)
    return (covariance[None], weights)


def solution(mesh):
    split = Mesh(mesh.devices.reshape(mesh.shape["chan"], 4, 4), ("chan", "tile_0", "tile_1"))
    return jax.shard_map(
        shards,
        mesh=split,
        in_specs=(P(None, None, TILE, "chan"), P("chan"), P("chan", None), P("chan", None)),
        out_specs=(P("chan", None, TILE, None), P("chan", None, None, TILE)),
        check_vma=False,
    )
```

```python
import functools
import math

import jax
import jax.numpy as jnp
from jax import lax
from jax.experimental import pallas as pl
from jax.experimental.pallas import tpu as pltpu
from jax.sharding import Mesh
from jax.sharding import PartitionSpec as P

ARRAY_ELEMENTS = 2048
SNAPSHOT_COUNT = 2048
SUBSPACE_SIZE = 32
BEAM_COUNT = 8
SUB_ITERS = 4
CG_ITERS = 12
TILE = ("tile_0", "tile_1")
TILES = 16
ROWS = 128
WIDE = 256


diagonal_loading = 0.1
f32 = jnp.float32
bf16 = jnp.bfloat16


def pieces(x, count=3):
    terms = [x.astype(bf16)]
    for _ in range(count - 1):
        x = x - terms[-1].astype(f32)
        terms.append(x.astype(bf16))
    return jnp.concatenate(terms, 0)


def fold(x, count):
    rows = x.shape[0] // count
    total = x[:rows]
    for n in range(1, count):
        total = total + x[n * rows : (n + 1) * rows]
    return total


def plain(a, b):
    return lax.dot_general(a, b, (((1,), (0,)), ((), ())), preferred_element_type=f32)


def turned_dot(a, b):
    return lax.dot_general(a, b, (((1,), (1,)), ((), ())), preferred_element_type=f32)


def tile_through(lhs, matrix, cols, count, sign):
    by_real = fold(plain(lhs[...], matrix[0, :, cols]), count)
    by_imag = fold(plain(lhs[...], matrix[1, :, cols]), count)
    half = by_real.shape[0] // 2
    swapped = jnp.concatenate([-by_imag[half:], by_imag[:half]], 0)
    return by_real + swapped if sign > 0 else by_real - swapped


def column_tiles():
    return [pl.ds(n * WIDE, WIDE) for n in range(ARRAY_ELEMENTS // WIDE)]


def beam_sum(x):
    folded = x[:BEAM_COUNT] + x[BEAM_COUNT:]
    return jnp.sum(folded, axis=1, keepdims=True)


def twice(x):
    return jnp.concatenate([x, x], 0)


def every_group(x):
    x = x + pltpu.roll(x, 64, 1)
    return x + pltpu.roll(x, 32, 1)


def stack_pieces(y):
    blank = jnp.zeros((SUBSPACE_SIZE, y.shape[1]), bf16)
    return jnp.concatenate(
        [pieces(y[:SUBSPACE_SIZE]), blank, pieces(y[SUBSPACE_SIZE:]), blank], 0
    )


def unit_rows(stacked, store):
    size = SUBSPACE_SIZE
    raw = turned_dot(stacked[...], stacked[...])
    top, bottom = fold(raw[: 4 * size], 4), fold(raw[4 * size :], 4)
    g_r = every_group(top[:, : 4 * size] + bottom[:, 4 * size :])
    g_i = every_group(bottom[:, : 4 * size] - top[:, 4 * size :])
    row = lax.broadcasted_iota(jnp.int32, (size, 4 * size), 0)
    lane = lax.broadcasted_iota(jnp.int32, (size, 4 * size), 1)
    a_r = jnp.where(lane < size, g_r, jnp.where(lane - size == row, 1.0, 0.0))
    a_i = jnp.where(lane < size, g_i, 0.0)
    blocks = size // 8
    a_r = [a_r[8 * n : 8 * n + 8] for n in range(blocks)]
    a_i = [a_i[8 * n : 8 * n + 8] for n in range(blocks)]
    within = lax.broadcasted_iota(jnp.int32, (8, 1), 0)
    pivots = []
    for k in range(size):
        own, at = k // 8, k % 8
        pivot = a_r[own][at : at + 1, k : k + 1]
        pivots.append(pivot)
        inverse = 1.0 / pivot
        p_r = a_r[own][at : at + 1] * inverse
        p_i = a_i[own][at : at + 1] * inverse
        for n in range((k + 1) // 8, blocks):
            f_r, f_i = a_r[n][:, k : k + 1], a_i[n][:, k : k + 1]
            if n == own:
                f_r = jnp.where(within > at, f_r, 0.0)
                f_i = jnp.where(within > at, f_i, 0.0)
            a_r[n], a_i[n] = (
                a_r[n] - (f_r * p_r - f_i * p_i),
                a_i[n] - (f_r * p_i + f_i * p_r),
            )
    scale = 1.0 / jnp.sqrt(jnp.concatenate(pivots, 0))
    middle = (lane >= size) & (lane < 2 * size)
    j_r = every_group(jnp.where(middle, jnp.concatenate(a_r, 0) * scale, 0.0))
    j_i = every_group(jnp.where(middle, jnp.concatenate(a_i, 0) * scale, 0.0))
    lhs = pieces(
        jnp.concatenate([jnp.concatenate([j_r, -j_i], 1), jnp.concatenate([j_i, j_r], 1)], 0)
    )
    for cols in column_tiles():
        store(cols, fold(plain(lhs, stacked[:, cols]), 3))


def weights_kernel(flag, place, picks, steering, *refs):
    gathered = refs[:TILES]
    cov_out, out = refs[TILES : TILES + 2]
    v, vt, basis, basis_t, wide, seen, narrow, cov, state, sems, out_sems = refs[TILES + 2 :]
    inverse_count = 1.0 / SNAPSHOT_COUNT
    tiles = column_tiles()

    def copy(block, part):
        outer, inner = block // 4, block % 4
        if part == 0:
            piece, half = gathered[2 * outer + inner // 2], inner % 2
        else:
            piece, half = gathered[8 + 2 * inner + outer // 2], outer % 2
        return pltpu.make_async_copy(
            piece.at[pl.ds(half * ROWS, ROWS)], v.at[part, pl.ds(block * ROWS, ROWS)], sems.at[block, part]
        )

    for n in range(TILES):
        for part in range(2):
            copy(n, part).start()

    exact_rows = wide.at[: 2 * SUBSPACE_SIZE]
    squares = jnp.zeros((8, ARRAY_ELEMENTS), f32)
    for n, cols in enumerate(tiles):
        for part in range(2):
            for block in (2 * n, 2 * n + 1):
                copy(block, part).wait()
            rows = v[part, n * WIDE : (n + 1) * WIDE, :]
            vt[part, :, cols] = rows.T
            exact = rows.astype(f32)
            squares = squares + jnp.sum((exact * exact).reshape(WIDE // 8, 8, ARRAY_ELEMENTS), axis=0)
        taken_r = plain(picks[...], vt[0, :, cols])
        taken_i = plain(picks[...], vt[1, :, cols])
        exact_rows[:, cols] = jnp.concatenate([taken_r, -taken_i], 0).astype(bf16)
    power = jnp.sum(jnp.sum(squares, axis=0, keepdims=True), axis=1, keepdims=True)
    load = diagonal_loading * (power * inverse_count) / ARRAY_ELEMENTS

    own = pl.ds(pl.multiple_of(place[0] * ROWS, ROWS), ROWS)

    def covariance_tiles(sweep_index):
        for n in range(2):
            cols = pl.ds(pl.multiple_of((2 * sweep_index + n) * WIDE, WIDE), WIDE)
            lhs = jnp.concatenate([vt[0, own, :], vt[1, own, :]], 0)
            by_real, by_imag = plain(lhs, v[0, :, cols]), plain(lhs, v[1, :, cols])
            cov[0, :, cols] = (by_real[:ROWS] + by_imag[ROWS:]) * inverse_count
            cov[1, :, cols] = (by_real[ROWS:] - by_imag[:ROWS]) * inverse_count

    def cov_copy(part):
        return pltpu.make_async_copy(cov.at[part], cov_out.at[part], out_sems.at[part])

    for cols in tiles:
        basis[:, cols] = stack_pieces(tile_through(exact_rows, v, cols, 1, 1) * inverse_count)

    def to_wide(cols, q):
        wide[:, cols] = pieces(q, 2)

    def sweep(n, carry):
        covariance_tiles(n)
        unit_rows(basis, to_wide)
        for cols in tiles:
            seen[:, cols] = pieces(tile_through(wide, vt, cols, 2, -1), 2)
        for cols in tiles:
            basis[:, cols] = stack_pieces(tile_through(seen, v, cols, 2, 1) * inverse_count)
        return carry

    lax.fori_loop(0, SUB_ITERS - 1, sweep, 0)
    covariance_tiles(SUB_ITERS - 1)
    for part in range(2):
        cov_copy(part).start()
    flagged = flag[0].astype(f32)

    def keep(cols, q):
        basis[:, cols] = stack_pieces(q * flagged)
        basis_t[cols, :] = basis[:, cols].T

    unit_rows(basis, keep)

    def coefficients(cols, x):
        return fold(plain(pieces(x), basis_t[cols, :]), 3)

    def remove(raw):
        half = BEAM_COUNT
        c_r = raw[:half, :128] + raw[half:, 128:]
        c_i = raw[half:, :128] - raw[:half, 128:]
        c = every_group(jnp.concatenate([c_r, c_i], 0))
        crossed = jnp.concatenate([-c[half:], c[:half]], 0)
        both = pieces(jnp.concatenate([c, crossed], 1))
        return jnp.concatenate([fold(plain(both, basis[:, cols]), 3) for cols in tiles], 1)

    source = steering[...]
    state[0] = jnp.zeros_like(source)
    held = remove(sum(coefficients(cols, steering[:, cols]) for cols in tiles))
    clean = source - held
    state[1] = clean
    state[2] = clean
    state[3] = held
    inside = beam_sum(held * held)

    def correlate(write):
        narrow[...] = pieces(state[2], 2)
        total = jnp.zeros((2 * BEAM_COUNT, WIDE), f32)
        for cols in tiles:
            part = tile_through(narrow, vt, cols, 2, -1)
            if write:
                seen[: 4 * BEAM_COUNT, cols] = pieces(part, 2)
            total = total + part * part
        return beam_sum(total)

    def curvature_of(energy, direction, tau):
        return energy * inverse_count + load * (
            beam_sum(direction * direction) + tau * tau * inside
        )

    def iterate(n, carry):
        norm, xi, rho, tau = carry
        energy = correlate(True)
        direction = state[2]
        step = norm / curvature_of(energy, direction, tau)
        state[0] = state[0] + twice(step) * direction
        state[1] = state[1] - twice(step * load) * direction
        xi = xi + step * tau
        rho = rho - step * (load * tau)
        raw = jnp.zeros((2 * BEAM_COUNT, WIDE), f32)
        for cols in tiles:
            mapped = tile_through(seen.at[: 4 * BEAM_COUNT], v, cols, 2, 1) * inverse_count
            raw = raw + coefficients(cols, mapped)
            state[4, :, cols] = mapped
        residual = state[1] - twice(step) * (state[4] - remove(raw))
        state[1] = residual
        fresh = beam_sum(residual * residual) + rho * rho * inside
        ratio = fresh / norm
        state[2] = residual + twice(ratio) * direction
        tau = rho + ratio * tau
        return fresh, xi, rho, tau

    one = jnp.ones((BEAM_COUNT, 1), f32)
    first = (beam_sum(source * source), jnp.zeros((BEAM_COUNT, 1), f32), one, one)
    norm, xi, rho, tau = lax.fori_loop(0, CG_ITERS - 1, iterate, first)
    direction = state[2]
    step = norm / curvature_of(correlate(False), direction, tau)
    solved = state[0] + twice(step) * direction + twice(xi + step * tau) * state[3]
    response = beam_sum(source * solved)
    state[0] = ARRAY_ELEMENTS * solved / twice(response)
    out[:, 0, :] = state[0, :BEAM_COUNT, own]
    out[:, 1, :] = state[0, BEAM_COUNT:, own]
    for part in range(2):
        cov_copy(part).wait()


def local_weights(flag, place, gathered, picks, steering, interpret=False):
    vmem = pl.BlockSpec(memory_space=pltpu.VMEM)
    smem = pl.BlockSpec(memory_space=pltpu.SMEM)
    hbm = pl.BlockSpec(memory_space=pl.ANY)
    return pl.pallas_call(
        weights_kernel,
        out_shape=(
            jax.ShapeDtypeStruct((2, ROWS, ARRAY_ELEMENTS), f32),
            jax.ShapeDtypeStruct((BEAM_COUNT, 2, ROWS), f32),
        ),
        in_specs=[smem, smem, vmem, vmem] + [hbm] * TILES,
        out_specs=(hbm, vmem),
        scratch_shapes=[
            pltpu.VMEM((2, SNAPSHOT_COUNT, ARRAY_ELEMENTS), bf16),
            pltpu.VMEM((2, ARRAY_ELEMENTS, SNAPSHOT_COUNT), bf16),
            pltpu.VMEM((8 * SUBSPACE_SIZE, ARRAY_ELEMENTS), bf16),
            pltpu.VMEM((ARRAY_ELEMENTS, 8 * SUBSPACE_SIZE), bf16),
            pltpu.VMEM((4 * SUBSPACE_SIZE, ARRAY_ELEMENTS), bf16),
            pltpu.VMEM((4 * SUBSPACE_SIZE, SNAPSHOT_COUNT), bf16),
            pltpu.VMEM((4 * BEAM_COUNT, ARRAY_ELEMENTS), bf16),
            pltpu.VMEM((2, ROWS, ARRAY_ELEMENTS), f32),
            pltpu.VMEM((5, 2 * BEAM_COUNT, ARRAY_ELEMENTS), f32),
            pltpu.SemaphoreType.DMA((TILES, 2)),
            pltpu.SemaphoreType.DMA((2,)),
        ],
        compiler_params=pltpu.CompilerParams(vmem_limit_bytes=58 << 20),
        interpret=interpret,
    )(flag, place, picks, steering, *gathered)


def ring_gather(block, first, second):
    onward = [(n, (n + 1) % 4) for n in range(4)]
    back = [(n, (n - 1) % 4) for n in range(4)]
    half = block.shape[0] // 2
    before = lax.ppermute(block, first, onward)
    after = lax.ppermute(block, first, back)
    across = (
        lax.ppermute(before[:half], first, onward),
        lax.ppermute(after[half:], first, back),
    )
    near = jnp.concatenate([block, before], 0)
    far = jnp.concatenate([after, *across], 0)
    near_before = lax.ppermute(near, second, onward)
    near_after = lax.ppermute(near, second, back)
    far_before = lax.ppermute(far, second, onward)
    far_after = lax.ppermute(far, second, back)
    near_across = lax.ppermute(near_before, second, onward)
    far_across = lax.ppermute(far_after, second, back)
    return [near, far, near_before, far_before, near_after, far_after, near_across, far_across]


def steering_table(beam_entries):
    element_index = jnp.arange(ARRAY_ELEMENTS, dtype=jnp.int32)
    steer_phases = (beam_entries[..., None] * element_index % ARRAY_ELEMENTS).astype(f32) * (
        2.0 * math.pi / ARRAY_ELEMENTS
    )
    return jnp.concatenate([jnp.cos(steer_phases), jnp.sin(steer_phases)], axis=0)


def shards(voltages, rfi_flags, beam_steer_index, start_columns):
    place = lax.axis_index(TILE)
    turned = lax.all_to_all(voltages, "chan", split_axis=0, concat_axis=3, tiled=True)
    gathered = ring_gather(turned[0, 0], "tile_1", "tile_0")
    gathered += ring_gather(turned[0, 1], "tile_0", "tile_1")
    picks = (start_columns[0][:, None] == jnp.arange(ARRAY_ELEMENTS, dtype=jnp.int32)).astype(bf16)
    steering = steering_table(beam_steer_index[0])
    covariance, weights = local_weights(
        rfi_flags, place[None].astype(jnp.int32), gathered, picks, steering
    )
    return (covariance[None], weights[None])


def solution(mesh):
    split = Mesh(mesh.devices.reshape(mesh.shape["chan"], 4, 4), ("chan", "tile_0", "tile_1"))
    return jax.shard_map(
        shards,
        mesh=split,
        in_specs=(P(None, None, TILE, "chan"), P("chan"), P("chan", None), P("chan", None)),
        out_specs=(P("chan", None, TILE, None), P("chan", None, None, TILE)),
        check_vma=False,
    )
```

```python
import math

import jax
import jax.numpy as jnp
from jax import lax
from jax.experimental import pallas as pl
from jax.experimental.pallas import tpu as pltpu
from jax.sharding import Mesh
from jax.sharding import PartitionSpec as P


ARRAY_ELEMENTS = 2048
SNAPSHOT_COUNT = 2048
SUBSPACE_SIZE = 32
BEAM_COUNT = 8
SUB_ITERS = 4
CG_ITERS = 12
TILE = ("tile_0", "tile_1")
TILES = 16
PIECES = 24
ROWS = 128
WIDE = 256


diagonal_loading = 0.1
f32 = jnp.float32
bf16 = jnp.bfloat16


def pieces(x, count=3):
    terms = [x.astype(bf16)]
    for _ in range(count - 1):
        x = x - terms[-1].astype(f32)
        terms.append(x.astype(bf16))
    return jnp.concatenate(terms, 0)


def fold(x, count):
    rows = x.shape[0] // count
    total = x[:rows]
    for n in range(1, count):
        total = total + x[n * rows : (n + 1) * rows]
    return total


def plain(a, b):
    return lax.dot_general(a, b, (((1,), (0,)), ((), ())), preferred_element_type=f32)


def turned_dot(a, b):
    return lax.dot_general(a, b, (((1,), (1,)), ((), ())), preferred_element_type=f32)


def tile_through(lhs, matrix, cols, count, sign):
    by_real = fold(plain(lhs[...], matrix[0, :, cols]), count)
    by_imag = fold(plain(lhs[...], matrix[1, :, cols]), count)
    half = by_real.shape[0] // 2
    swapped = jnp.concatenate([-by_imag[half:], by_imag[:half]], 0)
    return by_real + swapped if sign > 0 else by_real - swapped


def column_tiles():
    return [pl.ds(n * WIDE, WIDE) for n in range(ARRAY_ELEMENTS // WIDE)]


def beam_sum(x):
    folded = x[:BEAM_COUNT] + x[BEAM_COUNT:]
    return jnp.sum(folded, axis=1, keepdims=True)


def twice(x):
    return jnp.concatenate([x, x], 0)


def every_group(x):
    x = x + pltpu.roll(x, 64, 1)
    return x + pltpu.roll(x, 32, 1)


def stack_pieces(y):
    blank = jnp.zeros((SUBSPACE_SIZE, y.shape[1]), bf16)
    return jnp.concatenate(
        [pieces(y[:SUBSPACE_SIZE]), blank, pieces(y[SUBSPACE_SIZE:]), blank], 0
    )


def unit_rows(stacked, store):
    size = SUBSPACE_SIZE
    raw = turned_dot(stacked[...], stacked[...])
    top, bottom = fold(raw[: 4 * size], 4), fold(raw[4 * size :], 4)
    g_r = every_group(top[:, : 4 * size] + bottom[:, 4 * size :])
    g_i = every_group(bottom[:, : 4 * size] - top[:, 4 * size :])
    row = lax.broadcasted_iota(jnp.int32, (size, 4 * size), 0)
    lane = lax.broadcasted_iota(jnp.int32, (size, 4 * size), 1)
    a_r = jnp.where(lane < size, g_r, jnp.where(lane - size == row, 1.0, 0.0))
    a_i = jnp.where(lane < size, g_i, 0.0)
    blocks = size // 8
    a_r = [a_r[8 * n : 8 * n + 8] for n in range(blocks)]
    a_i = [a_i[8 * n : 8 * n + 8] for n in range(blocks)]
    within = lax.broadcasted_iota(jnp.int32, (8, 1), 0)
    pivots = []
    for k in range(size):
        own, at = k // 8, k % 8
        pivot = a_r[own][at : at + 1, k : k + 1]
        pivots.append(pivot)
        inverse = 1.0 / pivot
        p_r = a_r[own][at : at + 1] * inverse
        p_i = a_i[own][at : at + 1] * inverse
        for n in range((k + 1) // 8, blocks):
            f_r, f_i = a_r[n][:, k : k + 1], a_i[n][:, k : k + 1]
            if n == own:
                f_r = jnp.where(within > at, f_r, 0.0)
                f_i = jnp.where(within > at, f_i, 0.0)
            a_r[n], a_i[n] = (
                a_r[n] - (f_r * p_r - f_i * p_i),
                a_i[n] - (f_r * p_i + f_i * p_r),
            )
    scale = 1.0 / jnp.sqrt(jnp.concatenate(pivots, 0))
    middle = (lane >= size) & (lane < 2 * size)
    j_r = every_group(jnp.where(middle, jnp.concatenate(a_r, 0) * scale, 0.0))
    j_i = every_group(jnp.where(middle, jnp.concatenate(a_i, 0) * scale, 0.0))
    lhs = pieces(
        jnp.concatenate([jnp.concatenate([j_r, -j_i], 1), jnp.concatenate([j_i, j_r], 1)], 0)
    )
    for cols in column_tiles():
        store(cols, fold(plain(lhs, stacked[:, cols]), 3))


def weights_kernel(flag, place, picks, steering, *refs):
    gathered = refs[:PIECES]
    cov_out, out = refs[PIECES : PIECES + 2]
    v, vt, basis, basis_t, wide, seen, narrow, cov, state, sems, out_sems = refs[PIECES + 2 :]
    inverse_count = 1.0 / SNAPSHOT_COUNT
    tiles = column_tiles()

    def copy(block, part):
        outer, inner = block // 4, block % 4
        step, kind = (outer, inner) if part == 0 else (inner, outer)
        piece, half = gathered[PIECES // 2 * part + 3 * step + min(kind, 2)], max(kind - 2, 0)
        return pltpu.make_async_copy(
            piece.at[pl.ds(half * ROWS, ROWS)], v.at[part, pl.ds(block * ROWS, ROWS)], sems.at[block, part]
        )

    for n in range(TILES):
        for part in range(2):
            copy(n, part).start()

    exact_rows = wide.at[: 2 * SUBSPACE_SIZE]
    squares = jnp.zeros((8, ARRAY_ELEMENTS), f32)
    for n, cols in enumerate(tiles):
        for part in range(2):
            for block in (2 * n, 2 * n + 1):
                copy(block, part).wait()
            rows = v[part, n * WIDE : (n + 1) * WIDE, :]
            vt[part, :, cols] = rows.T
            exact = rows.astype(f32)
            squares = squares + jnp.sum((exact * exact).reshape(WIDE // 8, 8, ARRAY_ELEMENTS), axis=0)
        taken_r = plain(picks[...], vt[0, :, cols])
        taken_i = plain(picks[...], vt[1, :, cols])
        exact_rows[:, cols] = jnp.concatenate([taken_r, -taken_i], 0).astype(bf16)
    power = jnp.sum(jnp.sum(squares, axis=0, keepdims=True), axis=1, keepdims=True)
    load = diagonal_loading * (power * inverse_count) / ARRAY_ELEMENTS

    own = pl.ds(pl.multiple_of(place[0] * ROWS, ROWS), ROWS)

    def covariance_tiles(sweep_index):
        for n in range(2):
            cols = pl.ds(pl.multiple_of((2 * sweep_index + n) * WIDE, WIDE), WIDE)
            lhs = jnp.concatenate([vt[0, own, :], vt[1, own, :]], 0)
            by_real, by_imag = plain(lhs, v[0, :, cols]), plain(lhs, v[1, :, cols])
            cov[0, :, cols] = (by_real[:ROWS] + by_imag[ROWS:]) * inverse_count
            cov[1, :, cols] = (by_real[ROWS:] - by_imag[:ROWS]) * inverse_count

    def cov_copy(part):
        return pltpu.make_async_copy(cov.at[part], cov_out.at[part], out_sems.at[part])

    for cols in tiles:
        basis[:, cols] = stack_pieces(tile_through(exact_rows, v, cols, 1, 1) * inverse_count)

    def to_wide(cols, q):
        wide[:, cols] = pieces(q, 2)

    def sweep(n, carry):
        covariance_tiles(n)
        unit_rows(basis, to_wide)
        for cols in tiles:
            seen[:, cols] = pieces(tile_through(wide, vt, cols, 2, -1), 2)
        for cols in tiles:
            basis[:, cols] = stack_pieces(tile_through(seen, v, cols, 2, 1) * inverse_count)
        return carry

    lax.fori_loop(0, SUB_ITERS - 1, sweep, 0)
    covariance_tiles(SUB_ITERS - 1)
    for part in range(2):
        cov_copy(part).start()
    flagged = flag[0].astype(f32)

    def keep(cols, q):
        basis[:, cols] = stack_pieces(q * flagged)
        basis_t[cols, :] = basis[:, cols].T

    unit_rows(basis, keep)

    def coefficients(cols, x):
        return fold(plain(pieces(x), basis_t[cols, :]), 3)

    def remove(raw):
        half = BEAM_COUNT
        c_r = raw[:half, :128] + raw[half:, 128:]
        c_i = raw[half:, :128] - raw[:half, 128:]
        c = every_group(jnp.concatenate([c_r, c_i], 0))
        crossed = jnp.concatenate([-c[half:], c[:half]], 0)
        both = pieces(jnp.concatenate([c, crossed], 1))
        return jnp.concatenate([fold(plain(both, basis[:, cols]), 3) for cols in tiles], 1)

    source = steering[...]
    state[0] = jnp.zeros_like(source)
    held = remove(sum(coefficients(cols, steering[:, cols]) for cols in tiles))
    clean = source - held
    state[1] = clean
    state[2] = clean
    state[3] = held
    inside = beam_sum(held * held)

    def correlate():
        narrow[...] = pieces(state[2], 2)
        total = jnp.zeros((2 * BEAM_COUNT, WIDE), f32)
        for cols in tiles:
            part = tile_through(narrow, vt, cols, 2, -1)
            seen[: 4 * BEAM_COUNT, cols] = pieces(part, 2)
            total = total + part * part
        return beam_sum(total)

    def curvature_of(energy, direction, tau):
        return energy * inverse_count + load * (
            beam_sum(direction * direction) + tau * tau * inside
        )

    def advance(norm, rho, tau, step):
        direction = state[2]
        rho = rho - step * (load * tau)
        raw = jnp.zeros((2 * BEAM_COUNT, WIDE), f32)
        for cols in tiles:
            mapped = tile_through(seen.at[: 4 * BEAM_COUNT], v, cols, 2, 1) * inverse_count
            raw = raw + coefficients(cols, mapped)
            state[4, :, cols] = mapped
        residual = state[1] - twice(step) * (state[4] - remove(raw) + load * direction)
        state[1] = residual
        fresh = beam_sum(residual * residual) + rho * rho * inside
        ratio = fresh / norm
        state[2] = residual + twice(ratio) * direction
        return fresh, rho, rho + ratio * tau

    def iterate(n, carry):
        norm, xi, rho, tau = carry
        energy = correlate()
        direction = state[2]
        step = norm / curvature_of(energy, direction, tau)
        state[0] = state[0] + twice(step) * direction
        xi = xi + step * tau
        norm, rho, tau = lax.cond(
            n < CG_ITERS - 1, advance, lambda norm, rho, tau, step: (norm, rho, tau), norm, rho, tau, step
        )
        return norm, xi, rho, tau

    one = jnp.ones((BEAM_COUNT, 1), f32)
    first = (beam_sum(source * source), jnp.zeros((BEAM_COUNT, 1), f32), one, one)
    _, xi, _, _ = lax.fori_loop(0, CG_ITERS, iterate, first)
    solved = state[0] + twice(xi) * state[3]
    response = beam_sum(source * solved)
    state[0] = ARRAY_ELEMENTS * solved / twice(response)
    out[:, 0, :] = state[0, :BEAM_COUNT, own]
    out[:, 1, :] = state[0, BEAM_COUNT:, own]
    for part in range(2):
        cov_copy(part).wait()


def local_weights(flag, place, gathered, picks, steering, interpret=False):
    vmem = pl.BlockSpec(memory_space=pltpu.VMEM)
    smem = pl.BlockSpec(memory_space=pltpu.SMEM)
    hbm = pl.BlockSpec(memory_space=pl.ANY)
    return pl.pallas_call(
        weights_kernel,
        out_shape=(
            jax.ShapeDtypeStruct((2, ROWS, ARRAY_ELEMENTS), f32),
            jax.ShapeDtypeStruct((BEAM_COUNT, 2, ROWS), f32),
        ),
        in_specs=[smem, smem, vmem, vmem] + [hbm] * PIECES,
        out_specs=(hbm, vmem),
        scratch_shapes=[
            pltpu.VMEM((2, SNAPSHOT_COUNT, ARRAY_ELEMENTS), bf16),
            pltpu.VMEM((2, ARRAY_ELEMENTS, SNAPSHOT_COUNT), bf16),
            pltpu.VMEM((8 * SUBSPACE_SIZE, ARRAY_ELEMENTS), bf16),
            pltpu.VMEM((ARRAY_ELEMENTS, 8 * SUBSPACE_SIZE), bf16),
            pltpu.VMEM((4 * SUBSPACE_SIZE, ARRAY_ELEMENTS), bf16),
            pltpu.VMEM((4 * SUBSPACE_SIZE, SNAPSHOT_COUNT), bf16),
            pltpu.VMEM((4 * BEAM_COUNT, ARRAY_ELEMENTS), bf16),
            pltpu.VMEM((2, ROWS, ARRAY_ELEMENTS), f32),
            pltpu.VMEM((5, 2 * BEAM_COUNT, ARRAY_ELEMENTS), f32),
            pltpu.SemaphoreType.DMA((TILES, 2)),
            pltpu.SemaphoreType.DMA((2,)),
        ],
        compiler_params=pltpu.CompilerParams(vmem_limit_bytes=58 << 20),
        interpret=interpret,
    )(flag, place, picks, steering, *gathered)


def ring_gather(block, first, second):
    onward = [(n, (n + 1) % 4) for n in range(4)]
    back = [(n, (n - 1) % 4) for n in range(4)]
    half = block.shape[0] // 2

    def both_ways(x):
        return lax.ppermute(x, second, onward), lax.ppermute(x, second, back)

    before = lax.ppermute(block, first, onward)
    after = lax.ppermute(block, first, back)
    own_ways = both_ways(block)
    across = (lax.ppermute(before[:half], first, onward), lax.ppermute(after[half:], first, back))
    before_ways = both_ways(before)
    far = jnp.concatenate([after, *across], 0)
    far_ways = both_ways(far)
    own_across = lax.ppermute(own_ways[0], second, onward)
    before_across = lax.ppermute(before_ways[0], second, onward)
    far_across = lax.ppermute(far_ways[1], second, back)
    return [
        block, before, far,
        own_ways[0], before_ways[0], far_ways[0],
        own_ways[1], before_ways[1], far_ways[1],
        own_across, before_across, far_across,
    ]


def steering_table(beam_entries):
    element_index = jnp.arange(ARRAY_ELEMENTS, dtype=jnp.int32)
    steer_phases = (beam_entries[..., None] * element_index % ARRAY_ELEMENTS).astype(f32) * (
        2.0 * math.pi / ARRAY_ELEMENTS
    )
    return jnp.concatenate([jnp.cos(steer_phases), jnp.sin(steer_phases)], axis=0)


def shards(voltages, rfi_flags, beam_steer_index, start_columns):
    place = lax.axis_index(TILE)
    turned = lax.all_to_all(voltages, "chan", split_axis=0, concat_axis=3, tiled=True)
    gathered = ring_gather(turned[0, 0], "tile_1", "tile_0")
    gathered += ring_gather(turned[0, 1], "tile_0", "tile_1")
    picks = (start_columns[0][:, None] == jnp.arange(ARRAY_ELEMENTS, dtype=jnp.int32)).astype(bf16)
    steering = steering_table(beam_steer_index[0])
    covariance, weights = local_weights(
        rfi_flags, place[None].astype(jnp.int32), gathered, picks, steering
    )
    return (covariance[None], weights[None])


def solution(mesh):
    split = Mesh(mesh.devices.reshape(mesh.shape["chan"], 4, 4), ("chan", "tile_0", "tile_1"))
    return jax.shard_map(
        shards,
        mesh=split,
        in_specs=(P(None, None, TILE, "chan"), P("chan"), P("chan", None), P("chan", None)),
        out_specs=(P("chan", None, TILE, None), P("chan", None, None, TILE)),
        check_vma=False,
    )
```
